32 devices in a mesh: dp: 1 (over z), tp: 32 (over x, y, core).
Axes of the slice: x: 4, y: 4, z: 1, core: 2. Of those that a mesh axis runs over, the one named last changes fastest.
The devices are a block of a 4x4x8 slice.
Arguments:
- x: bfloat16 [5120, 7168], P(('dp', 'tp'))
- w_gate: bfloat16 [7168, 20480], P(None, 'tp')
- w_up: bfloat16 [7168, 20480], P(None, 'tp')
- w_down: bfloat16 [20480, 7168], P('tp')
Outputs:
- output: bfloat16 [5120, 7168], P(('dp', 'tp'))
All inputs are finite; a program needn't handle non-finite values.
Results may differ from the reference program's by a relative error of at most 0.016.
Values are sent between devices in bfloat16 or wider.
A program may use at most 768 MiB of HBM per device.

```python
import jax
import jax.numpy as jnp

ROWS = 5120
D = 7168
FF = 20480


def setup_inputs(seed: int = 0, part: int = 0) -> dict:
    kx, kg, ku, kd = jax.random.split(jax.random.key(seed), 4)
    drawn = {
        "x": jax.random.normal(jax.random.fold_in(kx, part), (ROWS, D), jnp.float32),
        "w_gate": jax.random.normal(kg, (D, FF), jnp.float32) * D**-0.5,
        "w_up": jax.random.normal(ku, (D, FF), jnp.float32) * D**-0.5,
        "w_down": jax.random.normal(kd, (FF, D), jnp.float32) * FF**-0.5,
    }
    return {k: v.astype(jnp.bfloat16) for k, v in drawn.items()}


def reference(x, w_gate, w_up, w_down):
    gate = jnp.dot(x, w_gate, preferred_element_type=jnp.float32)
    up = jnp.dot(x, w_up, preferred_element_type=jnp.float32)
    hidden = (jax.nn.silu(gate) * up).astype(jnp.bfloat16)
    return jnp.dot(hidden, w_down, preferred_element_type=jnp.float32).astype(jnp.bfloat16)
```

```python
import functools
import math

import jax
import jax.numpy as jnp
from jax import lax
from jax.experimental import pallas as pl
from jax.experimental.pallas import tpu as pltpu
from jax.sharding import PartitionSpec as P

RING = 4
LANES = 128
TILE = 512


def _offset(k):
    return k + lax.div(k, 2) - 2 * lax.div(k, 3)


def _place(j):
    p = lax.div(j + 4, 8)
    w0, w1, w2 = lax.div((1 - p) * (2 - p), 2), p * (2 - p), lax.div(p * (p - 1), 2)
    k = w0 * j + w1 * (lax.div(j + 4, 2) - 4) + w2 * (j - 12)
    return _offset(k), w1 * (3 - 2 * lax.rem(j, 2)) + 2 * w2


def _device(a, b, c):
    x = a * (1 - c) + b * c
    y = b * (1 - c) + a * c
    return (x * RING + y) * 2 + c


def _kernel(
    x, w_gate, w_up, w_down,
    y, xg, pb, rb, rh,
    wgu, wd, h, xb, stq, sto, ib,
    w_sem, x_send, x_recv, d_send, d_recv, p_send, p_recv, rb_send, rb_recv, rh_send, rh_recv, ld_sem,
):
    rows, cols = x.shape
    half = rows // 2
    chunks = w_gate.shape[1] // LANES
    blocks = RING * RING
    lo, hi = pl.ds(0, half), pl.ds(half, half)
    halves = (lo, hi)

    me = lax.axis_index("tp")
    c = lax.rem(me, 2)
    chip = lax.div(me, 2)
    px, py = lax.div(chip, RING), lax.rem(chip, RING)
    a = px * (1 - c) + py * c
    b = py * (1 - c) + px * c

    def turn(v, d):
        return lax.rem(v + d, RING)

    a_right, a_left = _device(turn(a, 1), b, c), _device(turn(a, RING - 1), b, c)
    b_right, b_left = _device(a, turn(b, 1), c), _device(a, turn(b, RING - 1), c)
    partner = me + 1 - 2 * c

    def own(j):
        da, db = _place(j)
        return _device(turn(a, da), turn(b, db), c)

    def theirs(j):
        da, db = _place(j)
        return _device(turn(b, da), turn(a, db), 1 - c)

    def remote(src, dst, send, recv, device):
        return pltpu.make_async_remote_copy(
            src_ref=src, dst_ref=dst, send_sem=send, recv_sem=recv,
            device_id={"tp": device}, device_id_type=pl.DeviceIdType.MESH,
        )

    def weight_copies():
        for n in range(chunks):
            part = pl.ds(n * LANES, LANES)
            yield pltpu.make_async_copy(w_gate.at[:, part], wgu.at[n, :, pl.ds(0, LANES)], w_sem.at[2 * n])
            yield pltpu.make_async_copy(w_up.at[:, part], wgu.at[n, :, pl.ds(LANES, LANES)], w_sem.at[2 * n + 1])
        yield pltpu.make_async_copy(w_down, wd, w_sem.at[2 * chunks])

    barrier = pltpu.get_barrier_semaphore()
    peers = (partner, a_right, a_left, b_right, b_left)
    for peer in peers:
        pl.semaphore_signal(barrier, inc=1, device_id={"tp": peer}, device_id_type=pl.DeviceIdType.MESH)
    pl.semaphore_wait(barrier, len(peers))

    def ring(src, block, i, j, device):
        return remote(src, xg.at[block, halves[i]], x_send.at[j, i], x_recv.at[j, i], device)

    def arrived(j, i):
        slot = xg.at[own(j), halves[i]]
        remote(slot, slot, x_send.at[j, i], x_recv.at[j, i], me).wait_recv()

    def both_ways(src, block, k):
        for i in (0, 1):
            ring(src.at[halves[i]], block, i, 4 + 2 * k, b_right).start()
            ring(src.at[halves[1 - i]], block, 1 - i, 5 + 2 * k, b_left).start()

    def hand_over(src, block, j):
        return remote(src, xg.at[block], d_send.at[j], d_recv.at[j], partner)

    for i in (0, 1):
        ring(x.at[halves[i]], me, i, 2, a_right).start()
        ring(x.at[halves[1 - i]], me, 1 - i, 1, a_left).start()
    hand_over(x, me, 0).start()
    for copy in weight_copies():
        copy.start()
    arrived(1, 1)
    ring(xg.at[own(1), hi], own(1), 1, 3, a_left).start()
    arrived(2, 0)
    ring(xg.at[own(2), lo], own(2), 0, 3, a_right).start()
    both_ways(x, me, 0)
    for copy in weight_copies():
        copy.wait()

    unroll = max(u for u in range(1, 8) if (cols // TILE) % u == 0)

    def down(block, first, count, adds, out):
        def body(i, _):
            for u in range(unroll):
                part = pl.ds(pl.multiple_of((i * unroll + u) * TILE, TILE), TILE)
                acc = jnp.dot(
                    h[block, pl.ds(first, count), :], wd[:, part], preferred_element_type=jnp.float32
                )
                edges = sorted({first, first + count} | {e for _, _, s, t in adds for e in (s, t)})
                for s, t in zip(edges, edges[1:]):
                    piece = acc[s - first : t - first]
                    for ref, row, s1, t1 in adds:
                        if s1 <= s and t <= t1:
                            piece += ref[pl.ds(row + s - s1, t - s), part].astype(jnp.float32)
                    out[pl.ds(s, t - s), part] = piece.astype(out.dtype)
            return 0

        lax.fori_loop(0, cols // (TILE * unroll), body, 0)

    def load(src, dst, sem):
        return pltpu.make_async_copy(src, dst, ld_sem.at[sem])

    def term_arrived(j):
        remote(pb.at[j], pb.at[j], p_send.at[0], p_recv.at[j], me).wait_recv()

    def sum_hop(src, whole, slot, device):
        dst, send, recv = (rb, rb_send, rb_recv) if whole else (rh, rh_send, rh_recv)
        return remote(src, dst.at[slot], send.at[slot], recv.at[slot], device)

    def last_hop(src, i, slot, device):
        s = 8 + 2 * (slot - 8) + i
        return remote(src, rb.at[slot, halves[i]], rb_send.at[s], rb_recv.at[s], device)

    def sum_arrived(whole, slot):
        dst = rb if whole else rh
        sum_hop(dst.at[slot], whole, slot, me).wait_recv()

    def step(s, _):
        mine, other = xb.at[pl.ds(0, rows)], xb.at[pl.ds(rows, rows)]
        stage = lax.rem(s, 2)

        @pl.when(s == 0)
        def _():
            load(x, mine, 0).start()

        @pl.when((s >= 1) & (s <= 3))
        def _():
            @pl.when(s == 1)
            def _():
                arrived(1, 0)

            @pl.when(s == 2)
            def _():
                arrived(2, 1)

            @pl.when(s == 3)
            def _():
                arrived(3, 0)
                arrived(3, 1)

            both_ways(xg.at[own(s)], own(s), s)

        @pl.when((s >= 4) & (s <= 11))
        def _():
            k = lax.div(s - 4, 2)

            @pl.when(lax.rem(s, 2) == 0)
            def _():
                arrived(s, 0)
                ring(xg.at[own(s), lo], own(s), 0, 12 + k, b_right).start()
                arrived(s, 1)

            @pl.when(lax.rem(s, 2) == 1)
            def _():
                arrived(s, 1)
                ring(xg.at[own(s), hi], own(s), 1, 12 + k, b_left).start()
                arrived(s, 0)

        @pl.when((s >= 12) & (s <= 15))
        def _():
            arrived(s, 0)
            arrived(s, 1)

        @pl.when((s >= 1) & (s <= 15))
        def _():
            load(xg.at[own(s)], mine, 0).start()
            hand_over(xg.at[own(s)], own(s), s).start()

        @pl.when((s >= 1) & (s <= 16))
        def _():
            block = theirs(s - 1)
            remote(xg.at[block], xg.at[block], d_send.at[s - 1], d_recv.at[s - 1], me).wait_recv()
            load(xg.at[block], other, 1).start()

        @pl.when(s >= 2)
        def _():
            j = s - 2
            copy = remote(stq.at[stage], pb.at[j], p_send.at[stage], p_recv.at[j], partner)

            @pl.when(s >= 4)
            def _():
                copy.wait_send()

            down(blocks + j, 0, rows, (), stq.at[stage])
            copy.start()

        @pl.when(s <= 15)
        def _():
            load(x, mine, 0).wait()

        @pl.when((s >= 1) & (s <= 16))
        def _():
            load(x, other, 1).wait()

        @pl.when(s <= 16)
        def _():
            for n in range(chunks):
                acc = jnp.dot(xb[...], wgu[n], preferred_element_type=jnp.float32)
                part = pl.ds(n * LANES, LANES)
                hid = (jax.nn.silu(acc[:, :LANES]) * acc[:, LANES:]).astype(h.dtype)

                h[s + (blocks + 1) * lax.div(s, blocks), :, part] = hid[:rows]
                h[lax.rem(s + blocks, blocks + 1) + blocks, :, part] = hid[rows:]

        @pl.when(s >= 14)
        def _():
            j, k = s - 2, s - 14
            term_arrived(j)
            load(pb.at[j], ib.at[0], 0).start()
            load(pb.at[j], ib.at[0], 0).wait()
            down(j, 0, rows, ((ib.at[0], 0, 0, rows),), sto.at[k])
            sum_hop(sto.at[k, lo], False, k, b_right).start()
            sum_hop(sto.at[k, hi], False, 4 + k, b_left).start()

        return 0

    lax.fori_loop(0, blocks + 2, step, 0)

    def near(i, _):
        k = lax.rem(i + 1, 4)
        right, left = 2 * lax.rem(i, 2), 2 * lax.rem(i, 2) + 1
        for d, slot in ((1, right), (0, left)):
            j = 4 + 2 * k + d
            came = k if d else 4 + k

            @pl.when(i < 2)
            def _():
                sum_hop(sto.at[slot, lo], False, slot, me).wait_send()
                sum_hop(sto.at[slot, hi], False, 4 + slot, me).wait_send()

            @pl.when(i >= 2)
            def _():
                sum_hop(sto.at[slot], True, (i - 1) + 4 * (1 - d), me).wait_send()

            term_arrived(j)
            first = load(pb.at[j], ib.at[0], 0)
            first.start()
            sum_arrived(False, came)
            second = load(rh.at[came], ib.at[1, lo], 1)
            second.start()
            first.wait()
            second.wait()
            part = (0, half) if d else (half, rows)
            down(j, 0, rows, ((ib.at[0], 0, 0, rows), (ib.at[1], 0, *part)), sto.at[slot])
            sum_hop(sto.at[slot], True, k if d else 4 + k, b_right if d else b_left).start()
        return 0

    lax.fori_loop(0, 4, near, 0)

    def gather_terms(k):
        term_arrived(k)
        sum_arrived(True, k)
        sum_arrived(True, 4 + k)
        copies = [load(pb.at[k], ib.at[0], 0), load(rb.at[k], ib.at[1], 1), load(rb.at[4 + k], ib.at[2], 2)]
        for copy in copies:
            copy.start()
        for copy in copies:
            copy.wait()

    three = tuple((ib.at[i], 0, 0, rows) for i in range(3))

    def rows_of(adds, s, t):
        return tuple((ref, s, s, t) for ref, _, _, _ in adds)

    sum_hop(sto.at[0], True, 3, me).wait_send()
    gather_terms(3)
    down(3, 0, rows, three, sto.at[0])
    sum_hop(sto.at[0, lo], False, 8, a_right).start()
    sum_hop(sto.at[0, hi], False, 9, a_left).start()

    sum_hop(sto.at[1], True, 7, me).wait_send()
    gather_terms(1)
    down(1, half, half, rows_of(three, half, rows), sto.at[1])
    last_hop(sto.at[1, hi], 1, 8, a_right).start()
    sum_arrived(False, 8)
    extra = load(rh.at[8], xb.at[lo], 3)
    extra.start()
    extra.wait()
    down(1, 0, half, rows_of(three, 0, half) + ((xb, 0, 0, half),), sto.at[1])
    last_hop(sto.at[1, lo], 0, 8, a_right).start()

    sum_hop(sto.at[2], True, 0, me).wait_send()
    gather_terms(2)
    down(2, 0, half, rows_of(three, 0, half), sto.at[2])
    last_hop(sto.at[2, lo], 0, 9, a_left).start()
    sum_arrived(False, 9)
    extra = load(rh.at[9], xb.at[lo], 3)
    extra.start()
    extra.wait()
    down(2, half, half, rows_of(three, half, rows) + ((xb, 0, half, rows),), sto.at[2])
    last_hop(sto.at[2, hi], 1, 9, a_left).start()

    sum_hop(sto.at[3], True, 4, me).wait_send()
    gather_terms(0)
    for slot in (8, 9):
        for i in (0, 1):
            last_hop(rb.at[slot, halves[i]], i, slot, me).wait_recv()
    extras = [load(rb.at[8 + i], xb.at[pl.ds(i * rows, rows)], 3 + i) for i in range(2)]
    for copy in extras:
        copy.start()
    for copy in extras:
        copy.wait()
    down(0, 0, rows, three + ((xb, 0, 0, rows), (xb, rows, 0, rows)), sto.at[3])
    out = load(sto.at[3], y, 0)
    out.start()

    for j in range(1, blocks):
        for i in (0, 1):
            remote(xg.at[0, lo], xg.at[0, lo], x_send.at[j, i], x_recv.at[j, i], me).wait_send()
    for j in range(blocks):
        remote(xg.at[0], xg.at[0], d_send.at[j], d_recv.at[j], me).wait_send()
    for stage in range(2):
        remote(stq.at[stage], pb.at[0], p_send.at[stage], p_recv.at[0], me).wait_send()
    for slot, part in ((8, lo), (9, hi)):
        sum_hop(sto.at[0, part], False, slot, me).wait_send()
    for slot in (8, 9):
        for i in (0, 1):
            last_hop(sto.at[slot - 7, halves[i]], i, slot, me).wait_send()
    out.wait()


def solution(mesh):
    n = mesh.shape["tp"]
    if n != 2 * RING * RING:
        raise ValueError("ring size")

    def block(x, w_gate, w_up, w_down):
        rows, cols = x.shape
        hidden = w_gate.shape[1]
        dma = pltpu.SemaphoreType.DMA
        chunks = hidden // LANES
        flops = 6 * n * rows * cols * hidden
        any_spec = pl.BlockSpec(memory_space=pl.ANY)
        out = pl.pallas_call(
            _kernel,
            out_shape=(
                jax.ShapeDtypeStruct((rows, cols), x.dtype),
                jax.ShapeDtypeStruct((n, rows, cols), x.dtype),
                jax.ShapeDtypeStruct((n // 2, rows, cols), x.dtype),
                jax.ShapeDtypeStruct((10, rows, cols), x.dtype),
                jax.ShapeDtypeStruct((10, rows // 2, cols), x.dtype),
            ),
            in_specs=[any_spec] * 4,
            out_specs=[any_spec] * 5,
            scratch_shapes=[
                pltpu.VMEM((chunks, cols, 2 * LANES), x.dtype),
                pltpu.VMEM((hidden, cols), x.dtype),
                pltpu.VMEM((n + 2, rows, hidden), x.dtype),
                pltpu.VMEM((2 * rows, cols), x.dtype),
                pltpu.VMEM((2, rows, cols), x.dtype),
                pltpu.VMEM((4, rows, cols), x.dtype),
                pltpu.VMEM((3, rows, cols), x.dtype),
                dma((2 * chunks + 1,)),
                dma((n // 2, 2)),
                dma((n // 2, 2)),
                dma((n // 2,)),
                dma((n // 2,)),
                dma((2,)),
                dma((n // 2,)),
                dma((12,)),
                dma((12,)),
                dma((10,)),
                dma((10,)),
                dma((5,)),
            ],
            compiler_params=pltpu.CompilerParams(
                collective_id=0, has_side_effects=True, vmem_limit_bytes=67_000_000
            ),
            cost_estimate=pl.CostEstimate(flops=flops, bytes_accessed=8 * n * rows * cols, transcendentals=0),
        )(x, w_gate, w_up, w_down)
        return out[0]

    return jax.shard_map(
        block,
        mesh=mesh,
        in_specs=(P(("dp", "tp"), None), P(None, "tp"), P(None, "tp"), P("tp", None)),
        out_specs=P(("dp", "tp"), None),
        check_vma=False,
    )
```

```python
import functools
import math

import jax
import jax.numpy as jnp
from jax import lax
from jax.experimental import pallas as pl
from jax.experimental.pallas import tpu as pltpu
from jax.sharding import PartitionSpec as P

RING = 4
LANES = 128
TILE = 512


def _offset(k):
    return k + lax.div(k, 2) - 2 * lax.div(k, 3)


def _place(j):
    p = lax.div(j + 4, 8)
    w0, w1, w2 = lax.div((1 - p) * (2 - p), 2), p * (2 - p), lax.div(p * (p - 1), 2)
    k = w0 * j + w1 * (lax.div(j + 4, 2) - 4) + w2 * (j - 12)
    return _offset(k), w1 * (3 - 2 * lax.rem(j, 2)) + 2 * w2


def _device(a, b, c):
    x = a * (1 - c) + b * c
    y = b * (1 - c) + a * c
    return (x * RING + y) * 2 + c


def _kernel(
    x, w_gate, w_up, w_down,
    y, xg, pb, rb, rh,
    wd, h, xb, stq, sto, ib,
    w_sem, x_send, x_recv, d_send, d_recv, p_send, p_recv, rb_send, rb_recv, rh_send, rh_recv, ld_sem, free,
):
    rows, cols = x.shape
    half = rows // 2
    chunks = w_gate.shape[1] // LANES
    blocks = RING * RING
    lo, hi = pl.ds(0, half), pl.ds(half, half)
    halves = (lo, hi)

    me = lax.axis_index("tp")
    c = lax.rem(me, 2)
    chip = lax.div(me, 2)
    px, py = lax.div(chip, RING), lax.rem(chip, RING)
    a = px * (1 - c) + py * c
    b = py * (1 - c) + px * c

    def turn(v, d):
        return lax.rem(v + d, RING)

    a_right, a_left = _device(turn(a, 1), b, c), _device(turn(a, RING - 1), b, c)
    b_right, b_left = _device(a, turn(b, 1), c), _device(a, turn(b, RING - 1), c)
    partner = me + 1 - 2 * c

    def own(j):
        da, db = _place(j)
        return _device(turn(a, da), turn(b, db), c)

    def theirs(j):
        da, db = _place(j)
        return _device(turn(b, da), turn(a, db), 1 - c)

    def remote(src, dst, send, recv, device):
        return pltpu.make_async_remote_copy(
            src_ref=src, dst_ref=dst, send_sem=send, recv_sem=recv,
            device_id={"tp": device}, device_id_type=pl.DeviceIdType.MESH,
        )

    def weight_copies(wgu):
        for n in range(chunks):
            part = pl.ds(n * LANES, LANES)
            yield pltpu.make_async_copy(w_gate.at[:, part], wgu.at[n, :, pl.ds(0, LANES)], w_sem.at[2 * n])
            yield pltpu.make_async_copy(w_up.at[:, part], wgu.at[n, :, pl.ds(LANES, LANES)], w_sem.at[2 * n + 1])
        yield pltpu.make_async_copy(w_down, wd, w_sem.at[2 * chunks])

    barrier = pltpu.get_barrier_semaphore()
    peers = (partner, a_right, a_left, b_right, b_left)
    for peer in peers:
        pl.semaphore_signal(barrier, inc=1, device_id={"tp": peer}, device_id_type=pl.DeviceIdType.MESH)
    with jax.named_scope("bar"):
        pl.semaphore_wait(barrier, len(peers))

    def ring(src, block, i, j, device):
        return remote(src, xg.at[block, halves[i]], x_send.at[j, i], x_recv.at[j, i], device)

    def arrived(j, i):
        slot = xg.at[own(j), halves[i]]
        remote(slot, slot, x_send.at[j, i], x_recv.at[j, i], me).wait_recv()

    def both_ways(src, block, k):
        for i in (0, 1):
            ring(src.at[halves[i]], block, i, 4 + 2 * k, b_right).start()
            ring(src.at[halves[1 - i]], block, 1 - i, 5 + 2 * k, b_left).start()

    def hand_over(src, block, j):
        return remote(src, xg.at[block], d_send.at[j], d_recv.at[j], partner)

    unroll = max(u for u in range(1, 8) if (cols // TILE) % u == 0)

    def columns(work):
        def body(i, _):
            for u in range(unroll):
                work(pl.ds(pl.multiple_of((i * unroll + u) * TILE, TILE), TILE))
            return 0

        lax.fori_loop(0, cols // (TILE * unroll), body, 0)

    def down(block, adds, outs):
        def work(part):
            acc = jnp.dot(h[block], wd[:, part], preferred_element_type=jnp.float32)
            edges = sorted({e for _, _, s, t in (*adds, *outs) for e in (s, t)})
            for s, t in zip(edges, edges[1:]):
                piece = acc[s:t]
                for ref, row, s1, t1 in adds:
                    if s1 <= s and t <= t1:
                        piece += ref[pl.ds(row + s - s1, t - s), part].astype(jnp.float32)
                for ref, row, s1, t1 in outs:
                    if s1 <= s and t <= t1:
                        ref[pl.ds(row + s - s1, t - s), part] = piece.astype(ref.dtype)

        columns(work)

    def total(refs, out):
        def work(part):
            acc = refs[0][:, part]
            for ref in refs[1:]:
                acc += ref[:, part].astype(jnp.float32)
            out[:, part] = acc.astype(out.dtype)

        columns(work)

    def load(src, dst, sem):
        return pltpu.make_async_copy(src, dst, ld_sem.at[sem])

    def term_arrived(j):
        remote(pb.at[j], pb.at[j], p_send.at[0], p_recv.at[j], me).wait_recv()

    def sum_hop(src, whole, slot, device):
        dst, send, recv = (rb, rb_send, rb_recv) if whole else (rh, rh_send, rh_recv)
        return remote(src, dst.at[slot], send.at[slot], recv.at[slot], device)

    def last_hop(src, i, slot, device):
        s = 8 + 2 * slot + i
        return remote(src, stq.at[slot, halves[i]], rb_send.at[s], rb_recv.at[s], device)

    def sum_arrived(whole, slot):
        dst = rb if whole else rh
        sum_hop(dst.at[slot], whole, slot, me).wait_recv()

    def gather(wgu):
        for i in (0, 1):
            ring(x.at[halves[i]], me, i, 2, a_right).start()
            ring(x.at[halves[1 - i]], me, 1 - i, 1, a_left).start()
        hand_over(x, me, 0).start()
        for copy in weight_copies(wgu):
            copy.start()
        arrived(1, 1)
        ring(xg.at[own(1), hi], own(1), 1, 3, a_left).start()
        arrived(2, 0)
        ring(xg.at[own(2), lo], own(2), 0, 3, a_right).start()
        both_ways(x, me, 0)
        for copy in weight_copies(wgu):
            copy.wait()

        def step(s, _):
            mine, other = xb.at[pl.ds(0, rows)], xb.at[pl.ds(rows, rows)]
            stage = lax.rem(s, 2)

            @pl.when(s == 0)
            def _():
                load(x, mine, 0).start()

            @pl.when((s >= 1) & (s <= 3))
            def _():
                with jax.named_scope("a0"):
                    @pl.when(s == 1)
                    def _():
                        arrived(1, 0)

                    @pl.when(s == 2)
                    def _():
                        arrived(2, 1)

                    @pl.when(s == 3)
                    def _():
                        arrived(3, 0)
                        arrived(3, 1)

                both_ways(xg.at[own(s)], own(s), s)

            @pl.when((s >= 4) & (s <= 11))
            def _():
                k = lax.div(s - 4, 2)

                @pl.when(lax.rem(s, 2) == 0)
                def _():
                    with jax.named_scope("a1"):
                        arrived(s, 0)
                        ring(xg.at[own(s), lo], own(s), 0, 12 + k, b_right).start()
                        arrived(s, 1)

                @pl.when(lax.rem(s, 2) == 1)
                def _():
                    with jax.named_scope("a2"):
                        arrived(s, 1)
                        ring(xg.at[own(s), hi], own(s), 1, 12 + k, b_left).start()
                        arrived(s, 0)

            @pl.when((s >= 12) & (s <= 15))
            def _():
                with jax.named_scope("a3"):
                    arrived(s, 0)
                    arrived(s, 1)

            @pl.when((s >= 1) & (s <= 15))
            def _():
                load(xg.at[own(s)], mine, 0).start()
                hand_over(xg.at[own(s)], own(s), s).start()

            @pl.when((s >= 1) & (s <= 16))
            def _():
                block = theirs(s - 1)
                remote(xg.at[block], xg.at[block], d_send.at[s - 1], d_recv.at[s - 1], me).wait_recv()
                load(xg.at[block], other, 1).start()

            @pl.when(s >= 2)
            def _():
                j = s - 2
                copy = remote(stq.at[stage], pb.at[j], p_send.at[stage], p_recv.at[j], partner)

                @pl.when(s >= 4)
                def _():
                    copy.wait_send()

                down(blocks + j, (), ((stq.at[stage], 0, 0, rows),))
                copy.start()

            @pl.when(s <= 15)
            def _():
                load(x, mine, 0).wait()

            @pl.when((s >= 1) & (s <= 16))
            def _():
                with jax.named_scope("lw"):
                    load(x, other, 1).wait()

            @pl.when(s <= 16)
            def _():
                for n in range(chunks):
                    acc = jnp.dot(xb[...], wgu[n], preferred_element_type=jnp.float32)
                    part = pl.ds(n * LANES, LANES)
                    hid = (jax.nn.silu(acc[:, :LANES]) * acc[:, LANES:]).astype(h.dtype)

                    h[s + (blocks + 1) * lax.div(s, blocks), :, part] = hid[:rows]
                    h[lax.rem(s + blocks, blocks + 1) + blocks, :, part] = hid[rows:]

            @pl.when(s >= 14)
            def _():
                j, k = s - 2, s - 14
                with jax.named_scope("s1w"):
                    term_arrived(j)
                    load(pb.at[j], ib.at[0], 0).start()
                    load(pb.at[j], ib.at[0], 0).wait()
                with jax.named_scope("s1d"):
                    down(j, ((ib.at[0], 0, 0, rows),), ((sto.at[k], 0, 0, rows),))
                sum_hop(sto.at[k, lo], False, k, b_right).start()
                sum_hop(sto.at[k, hi], False, 4 + k, b_left).start()

            return 0

        lax.fori_loop(0, blocks + 2, step, 0)

    pl.run_scoped(gather, pltpu.VMEM((chunks, cols, 2 * LANES), x.dtype))
    for stage in range(2):
        remote(stq.at[stage], pb.at[0], p_send.at[stage], p_recv.at[0], me).wait_send()
    for device in (a_left, a_right):
        pl.semaphore_signal(free, inc=1, device_id={"tp": device}, device_id_type=pl.DeviceIdType.MESH)

    def near(i, _):
        k = lax.rem(i + 1, 4)
        right, left = 2 * lax.rem(i, 2), 2 * lax.rem(i, 2) + 1
        for d, slot in ((1, right), (0, left)):
            j = 4 + 2 * k + d
            came = k if d else 4 + k

            @pl.when(i < 2)
            def _():
                sum_hop(sto.at[slot, lo], False, slot, me).wait_send()
                sum_hop(sto.at[slot, hi], False, 4 + slot, me).wait_send()

            @pl.when(i >= 2)
            def _():
                with jax.named_scope("nt"):
                    sum_hop(sto.at[slot], True, (i - 1) + 4 * (1 - d), me).wait_send()

            term_arrived(j)
            first = load(pb.at[j], ib.at[0], 0)
            first.start()
            sum_arrived(False, came)
            second = load(rh.at[came], ib.at[1, lo], 1)
            second.start()
            with jax.named_scope("nl"):
                first.wait()
                second.wait()
            part = (0, half) if d else (half, rows)
            down(j, ((ib.at[0], 0, 0, rows), (ib.at[1], 0, *part)), ((sto.at[slot], 0, 0, rows),))
            sum_hop(sto.at[slot], True, k if d else 4 + k, b_right if d else b_left).start()
        return 0

    lax.fori_loop(0, 4, near, 0)

    def gather_terms(k):
        term_arrived(k)
        sum_arrived(True, k)
        sum_arrived(True, 4 + k)
        copies = [load(pb.at[k], ib.at[0], 0), load(rb.at[k], ib.at[1], 1), load(rb.at[4 + k], ib.at[2], 2)]
        for copy in copies:
            copy.start()
        for copy in copies:
            copy.wait()

    three = tuple((ib.at[i], 0, 0, rows) for i in range(3))
    ends = (xb.at[pl.ds(0, rows)], xb.at[pl.ds(rows, rows)])

    def finish(acc):
        with jax.named_scope("t1"):
            gather_terms(1)
            down(1, three, ((acc, 0, 0, half), (ends[0], half, half, rows)))
        with jax.named_scope("t2"):
            gather_terms(2)
            down(2, three, ((ends[1], 0, 0, half), (acc, half, half, rows)))

        with jax.named_scope("t3w"):
            sum_hop(sto.at[0], True, 3, me).wait_send()
            gather_terms(3)
        with jax.named_scope("t3d"):
            down(3, three, ((sto.at[0], 0, 0, rows),))
        sum_hop(sto.at[0, lo], False, 8, a_right).start()
        sum_hop(sto.at[0, hi], False, 9, a_left).start()

        with jax.named_scope("fw"):
            pl.semaphore_wait(free, 2)
        last_hop(ends[0].at[hi], 1, 0, a_right).start()
        last_hop(ends[1].at[lo], 0, 1, a_left).start()
        for slot, i, device in ((0, 0, a_right), (1, 1, a_left)):
            with jax.named_scope("ew"):
                sum_arrived(False, 8 + slot)
            extra = load(rh.at[8 + slot], ib.at[slot, lo], 3 + slot)
            extra.start()
            extra.wait()
            with jax.named_scope("et"):
                total((acc.at[halves[i]], ib.at[slot, lo]), ends[slot].at[halves[i]])
            last_hop(ends[slot].at[halves[i]], i, slot, device).start()

        with jax.named_scope("t0w"):
            gather_terms(0)
        with jax.named_scope("t0d"):
            down(0, three, ((acc, 0, 0, rows),))
        with jax.named_scope("aw"):
            for slot, i in ((0, 1), (1, 0), (0, 0)):
                last_hop(stq.at[slot, halves[i]], i, slot, me).wait_recv()
        with jax.named_scope("ad"):
            total((acc.at[lo], stq.at[0, lo], stq.at[1, lo]), y.at[lo])
        with jax.named_scope("bw"):
            last_hop(stq.at[1, hi], 1, 1, me).wait_recv()
        with jax.named_scope("bd"):
            total((acc.at[hi], stq.at[0, hi], stq.at[1, hi]), y.at[hi])

    pl.run_scoped(finish, pltpu.VMEM((rows, cols), jnp.float32))

    for j in range(1, blocks):
        for i in (0, 1):
            remote(xg.at[0, lo], xg.at[0, lo], x_send.at[j, i], x_recv.at[j, i], me).wait_send()
    for j in range(blocks):
        remote(xg.at[0], xg.at[0], d_send.at[j], d_recv.at[j], me).wait_send()
    for slot in (7, 0, 4):
        sum_hop(sto.at[0], True, slot, me).wait_send()
    for slot, part in ((8, lo), (9, hi)):
        sum_hop(sto.at[0, part], False, slot, me).wait_send()
    for slot in (0, 1):
        for i in (0, 1):
            last_hop(ends[slot].at[halves[i]], i, slot, me).wait_send()


def solution(mesh):
    n = mesh.shape["tp"]
    if n != 2 * RING * RING:
        raise ValueError("ring size")

    def block(x, w_gate, w_up, w_down):
        rows, cols = x.shape
        hidden = w_gate.shape[1]
        dma = pltpu.SemaphoreType.DMA
        chunks = hidden // LANES
        flops = 6 * n * rows * cols * hidden
        any_spec = pl.BlockSpec(memory_space=pl.ANY)
        out = pl.pallas_call(
            _kernel,
            out_shape=(
                pltpu.VMEM((rows, cols), x.dtype),
                jax.ShapeDtypeStruct((n, rows, cols), x.dtype),
                jax.ShapeDtypeStruct((n // 2, rows, cols), x.dtype),
                jax.ShapeDtypeStruct((8, rows, cols), x.dtype),
                jax.ShapeDtypeStruct((10, rows // 2, cols), x.dtype),
            ),
            in_specs=[any_spec] * 4,
            out_specs=[pl.BlockSpec(memory_space=pltpu.VMEM)] + [any_spec] * 4,
            scratch_shapes=[
                pltpu.VMEM((hidden, cols), x.dtype),
                pltpu.VMEM((n + 2, rows, hidden), x.dtype),
                pltpu.VMEM((2 * rows, cols), x.dtype),
                pltpu.VMEM((2, rows, cols), x.dtype),
                pltpu.VMEM((4, rows, cols), x.dtype),
                pltpu.VMEM((3, rows, cols), x.dtype),
                dma((2 * chunks + 1,)),
                dma((n // 2, 2)),
                dma((n // 2, 2)),
                dma((n // 2,)),
                dma((n // 2,)),
                dma((2,)),
                dma((n // 2,)),
                dma((12,)),
                dma((12,)),
                dma((10,)),
                dma((10,)),
                dma((5,)),
                pltpu.SemaphoreType.REGULAR,
            ],
            compiler_params=pltpu.CompilerParams(
                collective_id=0, has_side_effects=True, vmem_limit_bytes=64_500_000
            ),
            cost_estimate=pl.CostEstimate(flops=flops, bytes_accessed=8 * n * rows * cols, transcendentals=0),
        )(x, w_gate, w_up, w_down)
        return out[0]

    return jax.shard_map(
        block,
        mesh=mesh,
        in_specs=(P(("dp", "tp"), None), P(None, "tp"), P(None, "tp"), P("tp", None)),
        out_specs=P(("dp", "tp"), None),
        check_vma=False,
    )
```

```python
import functools
import math

import jax
import jax.numpy as jnp
from jax import lax
from jax.experimental import pallas as pl
from jax.experimental.pallas import tpu as pltpu
from jax.sharding import PartitionSpec as P

RING = 4
LANES = 128
TILE = 512


def _offset(k):
    return k + lax.div(k, 2) - 2 * lax.div(k, 3)


def _place(j):
    p = lax.div(j + 4, 8)
    w0, w1, w2 = lax.div((1 - p) * (2 - p), 2), p * (2 - p), lax.div(p * (p - 1), 2)
    k = w0 * j + w1 * (lax.div(j + 4, 2) - 4) + w2 * (j - 12)
    return _offset(k), w1 * (3 - 2 * lax.rem(j, 2)) + 2 * w2


def _device(a, b, c):
    x = a * (1 - c) + b * c
    y = b * (1 - c) + a * c
    return (x * RING + y) * 2 + c


def _kernel(
    x, w_gate, w_up, w_down,
    y, xg, pb, rb, rh,
    wd, h, xb, stq, sto, ib,
    w_sem, x_send, x_recv, d_send, d_recv, p_send, p_recv, rb_send, rb_recv, rh_send, rh_recv, ld_sem, free,
):
    rows, cols = x.shape
    half = rows // 2
    chunks = w_gate.shape[1] // LANES
    blocks = RING * RING
    lo, hi = pl.ds(0, half), pl.ds(half, half)
    halves = (lo, hi)

    me = lax.axis_index("tp")
    c = lax.rem(me, 2)
    chip = lax.div(me, 2)
    px, py = lax.div(chip, RING), lax.rem(chip, RING)
    a = px * (1 - c) + py * c
    b = py * (1 - c) + px * c

    def turn(v, d):
        return lax.rem(v + d, RING)

    a_right, a_left = _device(turn(a, 1), b, c), _device(turn(a, RING - 1), b, c)
    b_right, b_left = _device(a, turn(b, 1), c), _device(a, turn(b, RING - 1), c)
    partner = me + 1 - 2 * c

    def own(j):
        da, db = _place(j)
        return _device(turn(a, da), turn(b, db), c)

    def theirs(j):
        da, db = _place(j)
        return _device(turn(b, da), turn(a, db), 1 - c)

    def remote(src, dst, send, recv, device):
        return pltpu.make_async_remote_copy(
            src_ref=src, dst_ref=dst, send_sem=send, recv_sem=recv,
            device_id={"tp": device}, device_id_type=pl.DeviceIdType.MESH,
        )

    def weight_copies(wgu):
        for n in range(chunks):
            part = pl.ds(n * LANES, LANES)
            yield pltpu.make_async_copy(w_gate.at[:, part], wgu.at[n, :, pl.ds(0, LANES)], w_sem.at[2 * n])
            yield pltpu.make_async_copy(w_up.at[:, part], wgu.at[n, :, pl.ds(LANES, LANES)], w_sem.at[2 * n + 1])
        yield pltpu.make_async_copy(w_down, wd, w_sem.at[2 * chunks])

    barrier = pltpu.get_barrier_semaphore()
    peers = (partner, a_right, a_left, b_right, b_left)
    for peer in peers:
        pl.semaphore_signal(barrier, inc=1, device_id={"tp": peer}, device_id_type=pl.DeviceIdType.MESH)
    with jax.named_scope("bar"):
        pl.semaphore_wait(barrier, len(peers))

    def ring(src, block, i, j, device):
        return remote(src, xg.at[block, halves[i]], x_send.at[j, i], x_recv.at[j, i], device)

    def arrived(j, i):
        slot = xg.at[own(j), halves[i]]
        remote(slot, slot, x_send.at[j, i], x_recv.at[j, i], me).wait_recv()

    def both_ways(src, block, k):
        for i in (0, 1):
            ring(src.at[halves[i]], block, i, 4 + 2 * k, b_right).start()
            ring(src.at[halves[1 - i]], block, 1 - i, 5 + 2 * k, b_left).start()

    def hand_over(src, block, j):
        return remote(src, xg.at[block], d_send.at[j], d_recv.at[j], partner)

    unroll = max(u for u in range(1, 8) if (cols // TILE) % u == 0)

    def columns(work):
        def body(i, _):
            for u in range(unroll):
                work(pl.ds(pl.multiple_of((i * unroll + u) * TILE, TILE), TILE))
            return 0

        lax.fori_loop(0, cols // (TILE * unroll), body, 0)

    def down(block, adds, outs):
        def work(part):
            acc = jnp.dot(h[block], wd[:, part], preferred_element_type=jnp.float32)
            edges = sorted({e for _, _, s, t in (*adds, *outs) for e in (s, t)})
            for s, t in zip(edges, edges[1:]):
                piece = acc[s:t]
                for ref, row, s1, t1 in adds:
                    if s1 <= s and t <= t1:
                        piece += ref[pl.ds(row + s - s1, t - s), part].astype(jnp.float32)
                for ref, row, s1, t1 in outs:
                    if s1 <= s and t <= t1:
                        ref[pl.ds(row + s - s1, t - s), part] = piece.astype(ref.dtype)

        columns(work)

    def total(refs, out):
        def work(part):
            acc = refs[0][:, part]
            for ref in refs[1:]:
                acc += ref[:, part].astype(jnp.float32)
            out[:, part] = acc.astype(out.dtype)

        columns(work)

    def load(src, dst, sem):
        return pltpu.make_async_copy(src, dst, ld_sem.at[sem])

    def term_arrived(j):
        remote(pb.at[j], pb.at[j], p_send.at[0], p_recv.at[j], me).wait_recv()

    def sum_hop(src, whole, slot, device):
        dst, send, recv = (rb, rb_send, rb_recv) if whole else (rh, rh_send, rh_recv)
        return remote(src, dst.at[slot], send.at[slot], recv.at[slot], device)

    def last_hop(src, i, slot, device):
        s = 8 + 2 * slot + i
        return remote(src, stq.at[slot, halves[i]], rb_send.at[s], rb_recv.at[s], device)

    def sum_arrived(whole, slot):
        dst = rb if whole else rh
        sum_hop(dst.at[slot], whole, slot, me).wait_recv()

    def gather(wgu):
        for i in (0, 1):
            ring(x.at[halves[i]], me, i, 2, a_right).start()
            ring(x.at[halves[1 - i]], me, 1 - i, 1, a_left).start()
        hand_over(x, me, 0).start()
        for copy in weight_copies(wgu):
            copy.start()
        arrived(1, 1)
        ring(xg.at[own(1), hi], own(1), 1, 3, a_left).start()
        arrived(2, 0)
        ring(xg.at[own(2), lo], own(2), 0, 3, a_right).start()
        both_ways(x, me, 0)
        for copy in weight_copies(wgu):
            copy.wait()

        def fetch_other(s):
            block = theirs(s - 1)
            with jax.named_scope("dw"):
                remote(xg.at[block], xg.at[block], d_send.at[s - 1], d_recv.at[s - 1], me).wait_recv()
            load(xg.at[block], xb.at[pl.ds(rows, rows)], 1).start()

        def project(s, first, last):
            for n in range(chunks):
                acc = jnp.dot(
                    xb[pl.ds(first * rows, (last - first) * rows), :], wgu[n], preferred_element_type=jnp.float32
                )
                hid = (jax.nn.silu(acc[:, :LANES]) * acc[:, LANES:]).astype(h.dtype)
                for i in range(first, last):
                    h[s + (blocks - 1) * i, :, pl.ds(n * LANES, LANES)] = hid[(i - first) * rows : (i - first + 1) * rows]

        def term(j):
            stage = lax.rem(j, 2)
            return remote(stq.at[stage], pb.at[j], p_send.at[stage], p_recv.at[j], partner)

        def hand_term(j):
            down(blocks + j, (), ((stq.at[lax.rem(j, 2)], 0, 0, rows),))
            term(j).start()

        def far(j):
            k = j - 12
            with jax.named_scope("s1w"):
                term_arrived(j)
                load(pb.at[j], ib.at[0], 2).start()
                load(pb.at[j], ib.at[0], 2).wait()
            with jax.named_scope("s1d"):
                down(j, ((ib.at[0], 0, 0, rows),), ((sto.at[k], 0, 0, rows),))
            sum_hop(sto.at[k, lo], False, k, b_right).start()
            sum_hop(sto.at[k, hi], False, 4 + k, b_left).start()

        def step(s, _):
            mine, other = xb.at[pl.ds(0, rows)], xb.at[pl.ds(rows, rows)]

            @pl.when(s == 0)
            def _():
                load(x, mine, 0).start()

            @pl.when((s >= 1) & (s <= 3))
            def _():
                with jax.named_scope("a0"):
                    @pl.when(s == 1)
                    def _():
                        arrived(1, 0)

                    @pl.when(s == 2)
                    def _():
                        arrived(2, 1)

                    @pl.when(s == 3)
                    def _():
                        arrived(3, 0)
                        arrived(3, 1)

                both_ways(xg.at[own(s)], own(s), s)

            @pl.when((s >= 4) & (s <= 11))
            def _():
                k = lax.div(s - 4, 2)

                @pl.when(lax.rem(s, 2) == 0)
                def _():
                    with jax.named_scope("a1"):
                        arrived(s, 0)
                        ring(xg.at[own(s), lo], own(s), 0, 12 + k, b_right).start()
                        arrived(s, 1)

                @pl.when(lax.rem(s, 2) == 1)
                def _():
                    with jax.named_scope("a2"):
                        arrived(s, 1)
                        ring(xg.at[own(s), hi], own(s), 1, 12 + k, b_left).start()
                        arrived(s, 0)

            @pl.when(s >= 12)
            def _():
                with jax.named_scope("a3"):
                    arrived(s, 0)
                    arrived(s, 1)

            @pl.when(s >= 1)
            def _():
                load(xg.at[own(s)], mine, 0).start()
                hand_over(xg.at[own(s)], own(s), s).start()

            @pl.when(s >= 1)
            def _():
                fetch_other(s)

            @pl.when(s >= 14)
            def _():
                far(s - 2)

            @pl.when(s == 0)
            def _():
                load(x, mine, 0).wait()
                project(s, 0, 1)

            @pl.when(s >= 1)
            def _():
                with jax.named_scope("lw"):
                    load(x, mine, 0).wait()
                    load(x, other, 1).wait()
                with jax.named_scope("gu"):
                    project(s, 0, 2)

                @pl.when(s >= 3)
                def _():
                    term(s - 1).wait_send()

                hand_term(s - 1)

            return 0

        lax.fori_loop(0, blocks, step, 0)

        other = xb.at[pl.ds(rows, rows)]
        fetch_other(blocks)
        load(x, other, 1).wait()
        with jax.named_scope("gh"):
            project(blocks, 1, 2)
        term(blocks - 1).wait_send()
        hand_term(blocks - 1)
        far(14)
        far(15)

    pl.run_scoped(gather, pltpu.VMEM((chunks, cols, 2 * LANES), x.dtype))
    for stage in range(2):
        remote(stq.at[stage], pb.at[0], p_send.at[stage], p_recv.at[0], me).wait_send()
    for device in (a_left, a_right):
        pl.semaphore_signal(free, inc=1, device_id={"tp": device}, device_id_type=pl.DeviceIdType.MESH)

    def near(i, _):
        k = lax.rem(i + 1, 4)
        right, left = 2 * lax.rem(i, 2), 2 * lax.rem(i, 2) + 1
        for d, slot in ((1, right), (0, left)):
            j = 4 + 2 * k + d
            came = k if d else 4 + k

            @pl.when(i < 2)
            def _():
                sum_hop(sto.at[slot, lo], False, slot, me).wait_send()
                sum_hop(sto.at[slot, hi], False, 4 + slot, me).wait_send()

            @pl.when(i >= 2)
            def _():
                with jax.named_scope("nt"):
                    sum_hop(sto.at[slot], True, (i - 1) + 4 * (1 - d), me).wait_send()

            term_arrived(j)
            first = load(pb.at[j], ib.at[0], 0)
            first.start()
            sum_arrived(False, came)
            second = load(rh.at[came], ib.at[1, lo], 1)
            second.start()
            with jax.named_scope("nl"):
                first.wait()
                second.wait()
            part = (0, half) if d else (half, rows)
            down(j, ((ib.at[0], 0, 0, rows), (ib.at[1], 0, *part)), ((sto.at[slot], 0, 0, rows),))
            sum_hop(sto.at[slot], True, k if d else 4 + k, b_right if d else b_left).start()
        return 0

    lax.fori_loop(0, 4, near, 0)

    def gather_terms(k):
        term_arrived(k)
        sum_arrived(True, k)
        sum_arrived(True, 4 + k)
        copies = [load(pb.at[k], ib.at[0], 0), load(rb.at[k], ib.at[1], 1), load(rb.at[4 + k], ib.at[2], 2)]
        for copy in copies:
            copy.start()
        for copy in copies:
            copy.wait()

    three = tuple((ib.at[i], 0, 0, rows) for i in range(3))
    ends = (xb.at[pl.ds(0, rows)], xb.at[pl.ds(rows, rows)])

    def finish(acc):
        with jax.named_scope("t1"):
            gather_terms(1)
            down(1, three, ((acc, 0, 0, half), (ends[0], half, half, rows)))
        with jax.named_scope("t2"):
            gather_terms(2)
            down(2, three, ((ends[1], 0, 0, half), (acc, half, half, rows)))

        for j in range(1, blocks):
            for i in (0, 1):
                remote(xg.at[0, lo], xg.at[0, lo], x_send.at[j, i], x_recv.at[j, i], me).wait_send()
        for j in range(blocks):
            remote(xg.at[0], xg.at[0], d_send.at[j], d_recv.at[j], me).wait_send()
        with jax.named_scope("t3w"):
            sum_hop(sto.at[0], True, 3, me).wait_send()
            gather_terms(3)
        with jax.named_scope("t3d"):
            down(3, three, ((sto.at[0], 0, 0, rows),))
        sum_hop(sto.at[0, lo], False, 8, a_right).start()
        sum_hop(sto.at[0, hi], False, 9, a_left).start()

        pl.semaphore_wait(free, 2)
        last_hop(ends[0].at[hi], 1, 0, a_right).start()
        last_hop(ends[1].at[lo], 0, 1, a_left).start()
        for slot, i, device in ((0, 0, a_right), (1, 1, a_left)):
            with jax.named_scope("ew"):
                sum_arrived(False, 8 + slot)
            extra = load(rh.at[8 + slot], ib.at[slot, lo], 3 + slot)
            extra.start()
            extra.wait()
            with jax.named_scope("et"):
                total((acc.at[halves[i]], ib.at[slot, lo]), ends[slot].at[halves[i]])
            last_hop(ends[slot].at[halves[i]], i, slot, device).start()

        with jax.named_scope("t0w"):
            gather_terms(0)
        with jax.named_scope("t0d"):
            down(0, three, ((acc, 0, 0, rows),))
        for slot in (7, 0, 4):
            sum_hop(sto.at[0], True, slot, me).wait_send()
        for slot, part in ((8, lo), (9, hi)):
            sum_hop(sto.at[0, part], False, slot, me).wait_send()
        for slot, i in ((0, 1), (1, 0)):
            with jax.named_scope("aw"):
                last_hop(stq.at[slot, halves[i]], i, slot, me).wait_recv()
                total((acc.at[halves[i]], stq.at[slot, halves[i]]), acc.at[halves[i]])
        for slot, i in ((0, 0), (1, 1)):
            with jax.named_scope("bw"):
                last_hop(stq.at[slot, halves[i]], i, slot, me).wait_recv()
                total((acc.at[halves[i]], stq.at[slot, halves[i]]), y.at[halves[i]])

    pl.run_scoped(finish, pltpu.VMEM((rows, cols), jnp.float32))

    for slot in (0, 1):
        for i in (0, 1):
            last_hop(ends[slot].at[halves[i]], i, slot, me).wait_send()


def solution(mesh):
    n = mesh.shape["tp"]
    if n != 2 * RING * RING:
        raise ValueError("ring size")

    def block(x, w_gate, w_up, w_down):
        rows, cols = x.shape
        hidden = w_gate.shape[1]
        dma = pltpu.SemaphoreType.DMA
        chunks = hidden // LANES
        flops = 6 * n * rows * cols * hidden
        any_spec = pl.BlockSpec(memory_space=pl.ANY)
        out = pl.pallas_call(
            _kernel,
            out_shape=(
                pltpu.VMEM((rows, cols), x.dtype),
                jax.ShapeDtypeStruct((n, rows, cols), x.dtype),
                jax.ShapeDtypeStruct((n // 2, rows, cols), x.dtype),
                jax.ShapeDtypeStruct((8, rows, cols), x.dtype),
                jax.ShapeDtypeStruct((10, rows // 2, cols), x.dtype),
            ),
            in_specs=[any_spec] * 4,
            out_specs=[pl.BlockSpec(memory_space=pltpu.VMEM)] + [any_spec] * 4,
            scratch_shapes=[
                pltpu.VMEM((hidden, cols), x.dtype),
                pltpu.VMEM((n, rows, hidden), x.dtype),
                pltpu.VMEM((2 * rows, cols), x.dtype),
                pltpu.VMEM((2, rows, cols), x.dtype),
                pltpu.VMEM((4, rows, cols), x.dtype),
                pltpu.VMEM((3, rows, cols), x.dtype),
                dma((2 * chunks + 1,)),
                dma((n // 2, 2)),
                dma((n // 2, 2)),
                dma((n // 2,)),
                dma((n // 2,)),
                dma((2,)),
                dma((n // 2,)),
                dma((12,)),
                dma((12,)),
                dma((10,)),
                dma((10,)),
                dma((5,)),
                pltpu.SemaphoreType.REGULAR,
            ],
            compiler_params=pltpu.CompilerParams(
                collective_id=0, has_side_effects=True, vmem_limit_bytes=64_500_000
            ),
            cost_estimate=pl.CostEstimate(flops=flops, bytes_accessed=8 * n * rows * cols, transcendentals=0),
        )(x, w_gate, w_up, w_down)
        return out[0]

    return jax.shard_map(
        block,
        mesh=mesh,
        in_specs=(P(("dp", "tp"), None), P(None, "tp"), P(None, "tp"), P("tp", None)),
        out_specs=P(("dp", "tp"), None),
        check_vma=False,
    )
```

```python
import functools
import math

import jax
import jax.numpy as jnp
from jax import lax
from jax.experimental import pallas as pl
from jax.experimental.pallas import tpu as pltpu
from jax.sharding import PartitionSpec as P

RING = 4
LANES = 128
TILE = 512


def _offset(k):
    return k + lax.div(k, 2) - 2 * lax.div(k, 3)


def _place(j):
    p = lax.div(j + 4, 8)
    w0, w1, w2 = lax.div((1 - p) * (2 - p), 2), p * (2 - p), lax.div(p * (p - 1), 2)
    k = w0 * j + w1 * (lax.div(j + 4, 2) - 4) + w2 * (j - 12)
    return _offset(k), w1 * (3 - 2 * lax.rem(j, 2)) + 2 * w2


def _device(a, b, c):
    x = a * (1 - c) + b * c
    y = b * (1 - c) + a * c
    return (x * RING + y) * 2 + c


def _kernel(
    x, w_gate, w_up, w_down,
    y, xg, pb, rb, rh,
    wd, h, xb, stq, sto, ib,
    w_sem, x_send, x_recv, d_send, d_recv, p_send, p_recv, rb_send, rb_recv, rh_send, rh_recv, ld_sem, free,
):
    rows, cols = x.shape
    half = rows // 2
    chunks = w_gate.shape[1] // LANES
    blocks = RING * RING
    lo, hi = pl.ds(0, half), pl.ds(half, half)
    halves = (lo, hi)

    me = lax.axis_index("tp")
    c = lax.rem(me, 2)
    chip = lax.div(me, 2)
    px, py = lax.div(chip, RING), lax.rem(chip, RING)
    a = px * (1 - c) + py * c
    b = py * (1 - c) + px * c

    def turn(v, d):
        return lax.rem(v + d, RING)

    a_right, a_left = _device(turn(a, 1), b, c), _device(turn(a, RING - 1), b, c)
    b_right, b_left = _device(a, turn(b, 1), c), _device(a, turn(b, RING - 1), c)
    partner = me + 1 - 2 * c

    def own(j):
        da, db = _place(j)
        return _device(turn(a, da), turn(b, db), c)

    def theirs(j):
        da, db = _place(j)
        return _device(turn(b, da), turn(a, db), 1 - c)

    def remote(src, dst, send, recv, device):
        return pltpu.make_async_remote_copy(
            src_ref=src, dst_ref=dst, send_sem=send, recv_sem=recv,
            device_id={"tp": device}, device_id_type=pl.DeviceIdType.MESH,
        )

    def weight_copies(wgu):
        for n in range(chunks):
            part = pl.ds(n * LANES, LANES)
            yield pltpu.make_async_copy(w_gate.at[:, part], wgu.at[n, :, pl.ds(0, LANES)], w_sem.at[0])
            yield pltpu.make_async_copy(w_up.at[:, part], wgu.at[n, :, pl.ds(LANES, LANES)], w_sem.at[0])
        yield pltpu.make_async_copy(w_down, wd, w_sem.at[1])

    barrier = pltpu.get_barrier_semaphore()
    peers = (partner, a_right, a_left, b_right, b_left)
    for peer in peers:
        pl.semaphore_signal(barrier, inc=1, device_id={"tp": peer}, device_id_type=pl.DeviceIdType.MESH)
    with jax.named_scope("bar"):
        pl.semaphore_wait(barrier, len(peers))

    def ring(src, block, i, j, device):
        return remote(src, xg.at[block, halves[i]], x_send.at[0], x_recv.at[2 * j - 2 + i], device)

    def arrived(j, i):
        slot = xg.at[own(j), halves[i]]
        remote(slot, slot, x_send.at[0], x_recv.at[2 * j - 2 + i], me).wait_recv()

    def both_ways(src, block, k):
        for i in (0, 1):
            ring(src.at[halves[i]], block, i, 4 + 2 * k, b_right).start()
            ring(src.at[halves[1 - i]], block, 1 - i, 5 + 2 * k, b_left).start()

    def hand_over(src, block, j):
        return remote(src, xg.at[block], d_send.at[0], d_recv.at[j], partner)

    unroll = max(u for u in range(1, 8) if (cols // TILE) % u == 0)

    def columns(work):
        def body(i, _):
            for u in range(unroll):
                work(pl.ds(pl.multiple_of((i * unroll + u) * TILE, TILE), TILE))
            return 0

        lax.fori_loop(0, cols // (TILE * unroll), body, 0)

    def down(block, adds, outs):
        def work(part):
            acc = jnp.dot(h[block], wd[:, part], preferred_element_type=jnp.float32)
            edges = sorted({e for _, _, s, t in (*adds, *outs) for e in (s, t)})
            for s, t in zip(edges, edges[1:]):
                piece = acc[s:t]
                for ref, row, s1, t1 in adds:
                    if s1 <= s and t <= t1:
                        piece += ref[pl.ds(row + s - s1, t - s), part].astype(jnp.float32)
                for ref, row, s1, t1 in outs:
                    if s1 <= s and t <= t1:
                        ref[pl.ds(row + s - s1, t - s), part] = piece.astype(ref.dtype)

        columns(work)

    def total(refs, out):
        def work(part):
            acc = refs[0][:, part]
            for ref in refs[1:]:
                acc += ref[:, part].astype(jnp.float32)
            out[:, part] = acc.astype(out.dtype)

        columns(work)

    def load(src, dst, sem):
        return pltpu.make_async_copy(src, dst, ld_sem.at[sem])

    def sum_hop(src, whole, slot, device):
        if whole:
            return remote(src, rb.at[slot], rb_send.at[slot], rb_recv.at[lax.rem(slot, 4)], device)
        send = lax.rem(slot, 4) if not isinstance(slot, int) else (slot % 4 if slot < 8 else 4)
        return remote(src, rh.at[slot], rh_send.at[send], rh_recv.at[slot], device)

    def halves_sent(k):
        remote(sto.at[0], rb.at[0], rh_send.at[k], rb_recv.at[0], me).wait_send()

    def last_hop(src, i, slot, device):
        return remote(src, stq.at[slot, halves[i]], rb_send.at[8], rb_recv.at[4 + 2 * slot + i], device)

    def half_arrived(slot):
        sum_hop(rh.at[slot], False, slot, me).wait_recv()

    def gather(wgu):
        for i in (0, 1):
            ring(x.at[halves[i]], me, i, 2, a_right).start()
            ring(x.at[halves[1 - i]], me, 1 - i, 1, a_left).start()
        hand_over(x, me, 0).start()
        for copy in weight_copies(wgu):
            copy.start()
        arrived(1, 1)
        ring(xg.at[own(1), hi], own(1), 1, 3, a_left).start()
        arrived(2, 0)
        ring(xg.at[own(2), lo], own(2), 0, 3, a_right).start()
        both_ways(x, me, 0)
        pltpu.make_async_copy(wgu, wgu, w_sem.at[0]).wait()
        pltpu.make_async_copy(w_down, wd, w_sem.at[1]).wait()

        def fetch_other(s):
            block = theirs(s - 1)
            remote(xg.at[block], xg.at[block], d_send.at[0], d_recv.at[s - 1], me).wait_recv()
            load(xg.at[block], xb.at[pl.ds(rows, rows)], 1).start()

        def project(s, first, last):
            for n in range(chunks):
                acc = jnp.dot(
                    xb[pl.ds(first * rows, (last - first) * rows), :], wgu[n], preferred_element_type=jnp.float32
                )
                hid = (jax.nn.silu(acc[:, :LANES]) * acc[:, LANES:]).astype(h.dtype)
                for i in range(first, last):
                    h[s + (blocks - 1) * i, :, pl.ds(n * LANES, LANES)] = hid[(i - first) * rows : (i - first + 1) * rows]

        def term(j, dst, sem):
            stage = lax.rem(j, 2)
            return remote(stq.at[stage], dst, p_send.at[stage], p_recv.at[sem], partner)

        def term_sent(j):
            term(j, pb.at[0], 0).wait_send()

        def hand_term(j):
            down(blocks + j, (), ((stq.at[lax.rem(j, 2)], 0, 0, rows),))
            if isinstance(j, int) and j == blocks - 1:
                term(j, pb.at[12], 4).start()
            elif isinstance(j, int):
                term(j, ib.at[j - 12], j - 11).start()
            else:
                @pl.when(j < 12)
                def _():
                    term(j, pb.at[j], 0).start()

                @pl.when(j >= 12)
                def _():
                    term(j, ib.at[j - 12], j - 11).start()

        def far(j):
            k = j - 12
            if isinstance(j, int) and j == blocks - 1:
                term(j, pb.at[12], 4).wait_recv()
                load(pb.at[12], ib.at[0], 2).start()
                load(pb.at[12], ib.at[0], 2).wait()
                came = ib.at[0]
            else:
                term(j, ib.at[k], k + 1).wait_recv()
                came = ib.at[k]
            down(j, ((came, 0, 0, rows),), ((sto.at[k], 0, 0, rows),))
            sum_hop(sto.at[k, lo], False, k, b_right).start()
            sum_hop(sto.at[k, hi], False, 4 + k, b_left).start()

        def step(s, _):
            mine, other = xb.at[pl.ds(0, rows)], xb.at[pl.ds(rows, rows)]

            @pl.when(s == 0)
            def _():
                load(x, mine, 0).start()

            @pl.when((s >= 1) & (s <= 3))
            def _():
                with jax.named_scope("a0"):
                    @pl.when(s == 1)
                    def _():
                        arrived(1, 0)

                    @pl.when(s == 2)
                    def _():
                        arrived(2, 1)

                    @pl.when(s == 3)
                    def _():
                        arrived(3, 0)
                        arrived(3, 1)

                both_ways(xg.at[own(s)], own(s), s)

            @pl.when((s >= 4) & (s <= 11))
            def _():
                k = lax.div(s - 4, 2)

                @pl.when(lax.rem(s, 2) == 0)
                def _():
                    with jax.named_scope("a1"):
                        arrived(s, 0)
                        ring(xg.at[own(s), lo], own(s), 0, 12 + k, b_right).start()
                        arrived(s, 1)

                @pl.when(lax.rem(s, 2) == 1)
                def _():
                    with jax.named_scope("a2"):
                        arrived(s, 1)
                        ring(xg.at[own(s), hi], own(s), 1, 12 + k, b_left).start()
                        arrived(s, 0)

            @pl.when(s >= 12)
            def _():
                with jax.named_scope("a3"):
                    arrived(s, 0)
                    arrived(s, 1)

            @pl.when(s >= 1)
            def _():
                load(xg.at[own(s)], mine, 0).start()
                hand_over(xg.at[own(s)], own(s), s).start()

            @pl.when(s >= 1)
            def _():
                fetch_other(s)

            @pl.when(s >= 2)
            def _():
                @pl.when(s >= 4)
                def _():
                    term_sent(s)

                hand_term(s - 2)

            load(x, mine, 0).wait()

            @pl.when(s >= 1)
            def _():
                load(x, other, 1).wait()

            project(s, 0, 2)

            @pl.when(s >= 14)
            def _():
                far(s - 2)

            return 0

        lax.fori_loop(0, blocks, step, 0)

        fetch_other(blocks)
        term_sent(blocks)
        hand_term(blocks - 2)
        load(x, xb.at[pl.ds(rows, rows)], 1).wait()
        with jax.named_scope("gh"):
            project(blocks, 1, 2)
        term_sent(blocks + 1)
        hand_term(blocks - 1)
        far(blocks - 2)
        far(blocks - 1)

    pl.run_scoped(gather, pltpu.VMEM((chunks, cols, 2 * LANES), x.dtype))
    for stage in range(2):
        remote(stq.at[stage], pb.at[0], p_send.at[stage], p_recv.at[0], me).wait_send()
    remote(pb.at[pl.ds(0, 12)], pb.at[pl.ds(0, 12)], p_send.at[0], p_recv.at[0], me).wait_recv()
    for device in (a_left, a_right):
        pl.semaphore_signal(free, inc=1, device_id={"tp": device}, device_id_type=pl.DeviceIdType.MESH)

    def near(i, _):
        k = lax.rem(i + 1, 4)
        right, left = 2 * lax.rem(i, 2), 2 * lax.rem(i, 2) + 1
        for d, slot in ((1, right), (0, left)):
            j = 4 + 2 * k + d
            came = k if d else 4 + k

            @pl.when(i < 2)
            def _():
                halves_sent(slot)

            @pl.when(i >= 2)
            def _():
                with jax.named_scope("nt"):
                    sum_hop(sto.at[slot], True, (i - 1) + 4 * (1 - d), me).wait_send()

            first = load(pb.at[j], ib.at[0], 0)
            first.start()
            half_arrived(came)
            second = load(rh.at[came], ib.at[1, lo], 1)
            second.start()
            with jax.named_scope("nl"):
                first.wait()
                second.wait()
            part = (0, half) if d else (half, rows)
            down(j, ((ib.at[0], 0, 0, rows), (ib.at[1], 0, *part)), ((sto.at[slot], 0, 0, rows),))
            sum_hop(sto.at[slot], True, k if d else 4 + k, b_right if d else b_left).start()
        return 0

    lax.fori_loop(0, 4, near, 0)

    def gather_terms(k):
        remote(rb.at[pl.ds(0, 2)], rb.at[pl.ds(0, 2)], rb_send.at[8], rb_recv.at[k], me).wait_recv()
        copies = [load(pb.at[k], ib.at[0], 0), load(rb.at[k], ib.at[1], 1), load(rb.at[4 + k], ib.at[2], 2)]
        for copy in copies:
            copy.start()
        for copy in copies:
            copy.wait()

    three = tuple((ib.at[i], 0, 0, rows) for i in range(3))
    ends = (xb.at[pl.ds(0, rows)], xb.at[pl.ds(rows, rows)])

    def finish(acc):
        with jax.named_scope("t1"):
            gather_terms(1)
            down(1, three, ((acc, 0, 0, half), (ends[0], half, half, rows)))
        with jax.named_scope("t2"):
            gather_terms(2)
            down(2, three, ((ends[1], 0, 0, half), (acc, half, half, rows)))

        sent = xg.at[pl.ds(0, blocks - 1)]
        remote(sent, sent, x_send.at[0], x_recv.at[0], me).wait_send()
        sent = xg.at[pl.ds(0, blocks)]
        remote(sent, sent, d_send.at[0], d_recv.at[0], me).wait_send()
        with jax.named_scope("t3w"):
            sum_hop(sto.at[0], True, 3, me).wait_send()
            gather_terms(3)
        with jax.named_scope("t3d"):
            down(3, three, ((sto.at[0], 0, 0, rows),))
        sum_hop(sto.at[0, lo], False, 8, a_right).start()
        sum_hop(sto.at[0, hi], False, 9, a_left).start()

        pl.semaphore_wait(free, 2)
        last_hop(ends[0].at[hi], 1, 0, a_right).start()
        last_hop(ends[1].at[lo], 0, 1, a_left).start()
        for slot, i, device in ((0, 0, a_right), (1, 1, a_left)):
            with jax.named_scope("ew"):
                half_arrived(8 + slot)
            extra = load(rh.at[8 + slot], ib.at[slot, lo], 3 + slot)
            extra.start()
            extra.wait()
            with jax.named_scope("et"):
                total((acc.at[halves[i]], ib.at[slot, lo]), ends[slot].at[halves[i]])
            last_hop(ends[slot].at[halves[i]], i, slot, device).start()

        with jax.named_scope("t0w"):
            gather_terms(0)
        with jax.named_scope("t0d"):
            down(0, three, ((acc, 0, 0, rows),))
        for slot in (7, 0, 4):
            sum_hop(sto.at[0], True, slot, me).wait_send()
        halves_sent(4)
        for slot, i in ((0, 1), (1, 0)):
            with jax.named_scope("aw"):
                last_hop(stq.at[slot, halves[i]], i, slot, me).wait_recv()
                total((acc.at[halves[i]], stq.at[slot, halves[i]]), acc.at[halves[i]])
        for slot, i in ((0, 0), (1, 1)):
            with jax.named_scope("bw"):
                last_hop(stq.at[slot, halves[i]], i, slot, me).wait_recv()
                total((acc.at[halves[i]], stq.at[slot, halves[i]]), y.at[halves[i]])

    pl.run_scoped(finish, pltpu.VMEM((rows, cols), jnp.float32))

    remote(sto.at[pl.ds(0, 2)], sto.at[pl.ds(0, 2)], rb_send.at[8], rb_recv.at[0], me).wait_send()


def solution(mesh):
    n = mesh.shape["tp"]
    if n != 2 * RING * RING:
        raise ValueError("ring size")

    def block(x, w_gate, w_up, w_down):
        rows, cols = x.shape
        hidden = w_gate.shape[1]
        dma = pltpu.SemaphoreType.DMA
        chunks = hidden // LANES
        flops = 6 * n * rows * cols * hidden
        any_spec = pl.BlockSpec(memory_space=pl.ANY)
        out = pl.pallas_call(
            _kernel,
            out_shape=(
                pltpu.VMEM((rows, cols), x.dtype),
                jax.ShapeDtypeStruct((n, rows, cols), x.dtype),
                jax.ShapeDtypeStruct((13, rows, cols), x.dtype),
                jax.ShapeDtypeStruct((8, rows, cols), x.dtype),
                jax.ShapeDtypeStruct((10, rows // 2, cols), x.dtype),
            ),
            in_specs=[any_spec] * 4,
            out_specs=[pl.BlockSpec(memory_space=pltpu.VMEM)] + [any_spec] * 4,
            scratch_shapes=[
                pltpu.VMEM((hidden, cols), x.dtype),
                pltpu.VMEM((n, rows, hidden), x.dtype),
                pltpu.VMEM((2 * rows, cols), x.dtype),
                pltpu.VMEM((2, rows, cols), x.dtype),
                pltpu.VMEM((4, rows, cols), x.dtype),
                pltpu.VMEM((3, rows, cols), x.dtype),
                dma((2,)),
                dma((1,)),
                dma((n - 2,)),
                dma((1,)),
                dma((n // 2,)),
                dma((2,)),
                dma((5,)),
                dma((9,)),
                dma((8,)),
                dma((5,)),
                dma((10,)),
                dma((5,)),
                pltpu.SemaphoreType.REGULAR,
            ],
            compiler_params=pltpu.CompilerParams(
                collective_id=0, has_side_effects=True, vmem_limit_bytes=64_500_000
            ),
            cost_estimate=pl.CostEstimate(flops=flops, bytes_accessed=8 * n * rows * cols, transcendentals=0),
        )(x, w_gate, w_up, w_down)
        return out[0]

    return jax.shard_map(
        block,
        mesh=mesh,
        in_specs=(P(("dp", "tp"), None), P(None, "tp"), P(None, "tp"), P("tp", None)),
        out_specs=P(("dp", "tp"), None),
        check_vma=False,
    )
```

```python
import functools
import math

import jax
import jax.numpy as jnp
from jax import lax
from jax.experimental import pallas as pl
from jax.experimental.pallas import tpu as pltpu
from jax.sharding import PartitionSpec as P

OFFSETS = (0, 1, 3, 2)
LANES = 128
TILE = 512


def _offset(k):
    return k + lax.div(k, 2) - 2 * lax.div(k, 3)


def _place(j):
    p = lax.div(j + 4, 8)
    w0, w1, w2 = lax.div((1 - p) * (2 - p), 2), p * (2 - p), lax.div(p * (p - 1), 2)
    k = w0 * j + w1 * (lax.div(j + 4, 2) - 4) + w2 * (j - 12)
    return _offset(k), w1 * (3 - 2 * lax.rem(j, 2)) + 2 * w2


def _device(ring, a, b, c):
    x = a * (1 - c) + b * c
    y = b * (1 - c) + a * c
    return (x * ring + y) * 2 + c


def _kernel(
    side,
    x, w_gate, w_up, w_down,
    y, xg, pb, rb, rh,
    wd, h, xb, stq, sto, ib,
    w_sem, x_send, x_recv, d_send, d_recv, p_send, p_recv, rb_send, rb_recv, rh_send, rh_recv, ld_sem, free,
):
    rows, cols = x.shape
    half = rows // 2
    chunks = w_gate.shape[1] // LANES
    blocks = side * side
    lo, hi = pl.ds(0, half), pl.ds(half, half)
    halves = (lo, hi)

    me = lax.axis_index("tp")
    c = lax.rem(me, 2)
    chip = lax.div(me, 2)
    px, py = lax.div(chip, side), lax.rem(chip, side)
    a = px * (1 - c) + py * c
    b = py * (1 - c) + px * c

    def turn(v, d):
        return lax.rem(v + d, side)

    a_right, a_left = _device(side, turn(a, 1), b, c), _device(side, turn(a, side - 1), b, c)
    b_right, b_left = _device(side, a, turn(b, 1), c), _device(side, a, turn(b, side - 1), c)
    partner = me + 1 - 2 * c

    def own(j):
        da, db = _place(j)
        return _device(side, turn(a, da), turn(b, db), c)

    def theirs(j):
        da, db = _place(j)
        return _device(side, turn(b, da), turn(a, db), 1 - c)

    def remote(src, dst, send, recv, device):
        return pltpu.make_async_remote_copy(
            src_ref=src, dst_ref=dst, send_sem=send, recv_sem=recv,
            device_id={"tp": device}, device_id_type=pl.DeviceIdType.MESH,
        )

    def weight_copies(wgu):
        for n in range(chunks):
            part = pl.ds(n * LANES, LANES)
            yield pltpu.make_async_copy(w_gate.at[:, part], wgu.at[n, :, pl.ds(0, LANES)], w_sem.at[0])
            yield pltpu.make_async_copy(w_up.at[:, part], wgu.at[n, :, pl.ds(LANES, LANES)], w_sem.at[0])
        yield pltpu.make_async_copy(w_down, wd, w_sem.at[1])

    barrier = pltpu.get_barrier_semaphore()
    peers = (partner, a_right, a_left, b_right, b_left)
    for peer in peers:
        pl.semaphore_signal(barrier, inc=1, device_id={"tp": peer}, device_id_type=pl.DeviceIdType.MESH)
    pl.semaphore_wait(barrier, len(peers))

    def ring(src, block, i, j, device):
        return remote(src, xg.at[block, halves[i]], x_send.at[0], x_recv.at[2 * j - 2 + i], device)

    def ring_end(src, block, i, k, device):
        return remote(src, xg.at[block, halves[i]], x_send.at[0], x_recv.at[22 + k], device)

    def arrived(j, i):
        slot = xg.at[own(j), halves[i]]
        remote(slot, slot, x_send.at[0], x_recv.at[2 * j - 2 + i], me).wait_recv()

    def both_ways(src, block, k):
        for i in (0, 1):
            ring(src.at[halves[i]], block, i, 4 + 2 * k, b_right).start()
            ring(src.at[halves[1 - i]], block, 1 - i, 5 + 2 * k, b_left).start()

    def hand_over(src, block, j):
        return remote(src, xg.at[block], d_send.at[0], d_recv.at[lax.rem(j, 4)], partner)

    unroll = max(u for u in range(1, 8) if (cols // TILE) % u == 0)

    def columns(work):
        def body(i, _):
            for u in range(unroll):
                work(pl.ds(pl.multiple_of((i * unroll + u) * TILE, TILE), TILE))
            return 0

        lax.fori_loop(0, cols // (TILE * unroll), body, 0)

    def down(block, adds, outs):
        def work(part):
            acc = jnp.dot(h[block], wd[:, part], preferred_element_type=jnp.float32)
            edges = sorted({e for _, _, s, t in (*adds, *outs) for e in (s, t)})
            for s, t in zip(edges, edges[1:]):
                piece = acc[s:t]
                for ref, row, s1, t1 in adds:
                    if s1 <= s and t <= t1:
                        piece += ref[pl.ds(row + s - s1, t - s), part].astype(jnp.float32)
                for ref, row, s1, t1 in outs:
                    if s1 <= s and t <= t1:
                        ref[pl.ds(row + s - s1, t - s), part] = piece.astype(ref.dtype)

        columns(work)

    def total(refs, out):
        def work(part):
            acc = refs[0][:, part]
            for ref in refs[1:]:
                acc += ref[:, part].astype(jnp.float32)
            out[:, part] = acc.astype(out.dtype)

        columns(work)

    def load(src, dst, sem):
        return pltpu.make_async_copy(src, dst, ld_sem.at[sem])

    def sum_hop(src, whole, slot, device):
        if whole:
            return remote(src, rb.at[slot], rb_send.at[slot], rb_recv.at[lax.rem(slot, 4)], device)
        send = lax.rem(slot, 4) if not isinstance(slot, int) else (slot % 4 if slot < 8 else 4)
        return remote(src, rh.at[slot], rh_send.at[send], rh_recv.at[slot], device)

    def halves_sent(k):
        remote(sto.at[0], rb.at[0], rh_send.at[k], rb_recv.at[0], me).wait_send()

    def last_hop(src, i, slot, device):
        return remote(src, stq.at[slot, halves[i]], rb_send.at[8], rb_recv.at[4 + 2 * slot + i], device)

    def half_arrived(slot):
        sum_hop(rh.at[slot], False, slot, me).wait_recv()

    def gather(wgu):
        for i in (0, 1):
            ring(x.at[halves[i]], me, i, 2, a_right).start()
            ring(x.at[halves[1 - i]], me, 1 - i, 1, a_left).start()
        hand_over(x, me, 0).start()
        for copy in weight_copies(wgu):
            copy.start()
        arrived(1, 1)
        ring(xg.at[own(1), hi], own(1), 1, 3, a_left).start()
        arrived(2, 0)
        ring(xg.at[own(2), lo], own(2), 0, 3, a_right).start()
        both_ways(x, me, 0)
        pltpu.make_async_copy(wgu, wgu, w_sem.at[0]).wait()
        pltpu.make_async_copy(w_down, wd, w_sem.at[1]).wait()

        def fetch_other(s):
            block = theirs(s - 1)
            remote(xg.at[block], xg.at[block], d_send.at[0], d_recv.at[lax.rem(s - 1, 4)], me).wait_recv()
            load(xg.at[block], xb.at[pl.ds(rows, rows)], 1).start()

        def project(s, first, last):
            for n in range(chunks):
                acc = jnp.dot(
                    xb[pl.ds(first * rows, (last - first) * rows), :], wgu[n], preferred_element_type=jnp.float32
                )
                hid = (jax.nn.silu(acc[:, :LANES]) * acc[:, LANES:]).astype(h.dtype)
                for i in range(first, last):
                    h[s + (blocks - 1) * i, :, pl.ds(n * LANES, LANES)] = hid[(i - first) * rows : (i - first + 1) * rows]

        def term(j, dst, sem):
            stage = lax.rem(j, 2)
            return remote(stq.at[stage], dst, p_send.at[stage], p_recv.at[sem], partner)

        def term_sent(j):
            term(j, pb.at[0], 0).wait_send()

        def hand_term(j):
            down(blocks + j, (), ((stq.at[lax.rem(j, 2)], 0, 0, rows),))
            if isinstance(j, int) and j == blocks - 1:
                term(j, pb.at[12], 4).start()
            elif isinstance(j, int):
                term(j, ib.at[j - 12], j - 11).start()
            else:
                @pl.when(j < 12)
                def _():
                    term(j, pb.at[j], 0).start()

                @pl.when(j >= 12)
                def _():
                    term(j, ib.at[j - 12], j - 11).start()

        def far(j):
            k = j - 12
            if isinstance(j, int) and j == blocks - 1:
                term(j, pb.at[12], 4).wait_recv()
                load(pb.at[12], ib.at[0], 2).start()
                load(pb.at[12], ib.at[0], 2).wait()
                came = ib.at[0]
            else:
                term(j, ib.at[k], k + 1).wait_recv()
                came = ib.at[k]
            down(j, ((came, 0, 0, rows),), ((sto.at[k], 0, 0, rows),))
            sum_hop(sto.at[k, lo], False, k, b_right).start()
            sum_hop(sto.at[k, hi], False, 4 + k, b_left).start()

        def step(s, _):
            mine, other = xb.at[pl.ds(0, rows)], xb.at[pl.ds(rows, rows)]

            @pl.when(s == 0)
            def _():
                load(x, mine, 0).start()

            @pl.when((s >= 1) & (s <= 3))
            def _():
                @pl.when(s == 1)
                def _():
                    arrived(1, 0)

                @pl.when(s == 2)
                def _():
                    arrived(2, 1)

                @pl.when(s == 3)
                def _():
                    arrived(3, 0)
                    arrived(3, 1)

                both_ways(xg.at[own(s)], own(s), s)

            @pl.when((s >= 4) & (s <= 11))
            def _():
                k = lax.div(s - 4, 2)

                @pl.when(lax.rem(s, 2) == 0)
                def _():
                    arrived(s, 0)
                    ring_end(xg.at[own(s), lo], own(s), 0, k, b_right).start()
                    arrived(s, 1)

                @pl.when(lax.rem(s, 2) == 1)
                def _():
                    arrived(s, 1)
                    ring_end(xg.at[own(s), hi], own(s), 1, k, b_left).start()
                    arrived(s, 0)

            @pl.when(s >= 12)
            def _():
                block = xg.at[own(s)]
                remote(block, block, x_send.at[0], x_recv.at[22 + s - 12], me).wait_recv()

            @pl.when(s >= 1)
            def _():
                load(xg.at[own(s)], mine, 0).start()
                hand_over(xg.at[own(s)], own(s), s).start()

            @pl.when(s >= 1)
            def _():
                fetch_other(s)

            @pl.when(s >= 2)
            def _():
                @pl.when(s >= 4)
                def _():
                    term_sent(s)

                hand_term(s - 2)

            load(x, mine, 0).wait()

            @pl.when(s >= 1)
            def _():
                load(x, other, 1).wait()

            project(s, 0, 2)

            @pl.when(s >= 14)
            def _():
                far(s - 2)

            return 0

        lax.fori_loop(0, blocks, step, 0)

        fetch_other(blocks)
        term_sent(blocks)
        hand_term(blocks - 2)
        load(x, xb.at[pl.ds(rows, rows)], 1).wait()
        project(blocks, 1, 2)
        term_sent(blocks + 1)
        hand_term(blocks - 1)
        far(blocks - 2)
        far(blocks - 1)

    pl.run_scoped(gather, pltpu.VMEM((chunks, cols, 2 * LANES), x.dtype))
    for stage in range(2):
        remote(stq.at[stage], pb.at[0], p_send.at[stage], p_recv.at[0], me).wait_send()
    remote(pb.at[pl.ds(0, 12)], pb.at[pl.ds(0, 12)], p_send.at[0], p_recv.at[0], me).wait_recv()
    for device in (a_left, a_right):
        pl.semaphore_signal(free, inc=1, device_id={"tp": device}, device_id_type=pl.DeviceIdType.MESH)

    def near(i, _):
        k = lax.rem(i + 1, 4)
        right, left = 2 * lax.rem(i, 2), 2 * lax.rem(i, 2) + 1
        for d, slot in ((1, right), (0, left)):
            j = 4 + 2 * k + d
            came = k if d else 4 + k

            @pl.when(i < 2)
            def _():
                halves_sent(slot)

            @pl.when(i >= 2)
            def _():
                sum_hop(sto.at[slot], True, (i - 1) + 4 * (1 - d), me).wait_send()

            first = load(pb.at[j], ib.at[0], 0)
            first.start()
            half_arrived(came)
            second = load(rh.at[came], ib.at[1, lo], 1)
            second.start()
            first.wait()
            second.wait()
            part = (0, half) if d else (half, rows)
            down(j, ((ib.at[0], 0, 0, rows), (ib.at[1], 0, *part)), ((sto.at[slot], 0, 0, rows),))
            sum_hop(sto.at[slot], True, k if d else 4 + k, b_right if d else b_left).start()
        return 0

    lax.fori_loop(0, 4, near, 0)

    def gather_terms(k):
        remote(rb.at[pl.ds(0, 2)], rb.at[pl.ds(0, 2)], rb_send.at[8], rb_recv.at[k], me).wait_recv()
        copies = [load(pb.at[k], ib.at[0], 0), load(rb.at[k], ib.at[1], 1), load(rb.at[4 + k], ib.at[2], 2)]
        for copy in copies:
            copy.start()
        for copy in copies:
            copy.wait()

    three = tuple((ib.at[i], 0, 0, rows) for i in range(3))
    ends = (xb.at[pl.ds(0, rows)], xb.at[pl.ds(rows, rows)])

    def finish(acc):
        gather_terms(1)
        down(1, three, ((acc, 0, 0, half), (ends[0], half, half, rows)))
        gather_terms(2)
        down(2, three, ((ends[1], 0, 0, half), (acc, half, half, rows)))

        sent = xg.at[pl.ds(0, blocks - 1)]
        remote(sent, sent, x_send.at[0], x_recv.at[0], me).wait_send()
        sent = xg.at[pl.ds(0, blocks)]
        remote(sent, sent, d_send.at[0], d_recv.at[0], me).wait_send()
        sum_hop(sto.at[0], True, 3, me).wait_send()
        gather_terms(3)
        down(3, three, ((sto.at[0], 0, 0, rows),))
        sum_hop(sto.at[0, lo], False, 8, a_right).start()
        sum_hop(sto.at[0, hi], False, 9, a_left).start()

        pl.semaphore_wait(free, 2)
        last_hop(ends[0].at[hi], 1, 0, a_right).start()
        last_hop(ends[1].at[lo], 0, 1, a_left).start()
        for slot, i, device in ((0, 0, a_right), (1, 1, a_left)):
            half_arrived(8 + slot)
            extra = load(rh.at[8 + slot], ib.at[slot, lo], 3 + slot)
            extra.start()
            extra.wait()
            total((acc.at[halves[i]], ib.at[slot, lo]), ends[slot].at[halves[i]])
            last_hop(ends[slot].at[halves[i]], i, slot, device).start()

        gather_terms(0)
        down(0, three, ((acc, 0, 0, rows),))
        for slot in (7, 0, 4):
            sum_hop(sto.at[0], True, slot, me).wait_send()
        halves_sent(4)
        for slot, i in ((0, 1), (1, 0)):
            last_hop(stq.at[slot, halves[i]], i, slot, me).wait_recv()
            total((acc.at[halves[i]], stq.at[slot, halves[i]]), acc.at[halves[i]])
        for slot, i in ((0, 0), (1, 1)):
            last_hop(stq.at[slot, halves[i]], i, slot, me).wait_recv()
            total((acc.at[halves[i]], stq.at[slot, halves[i]]), y.at[halves[i]])

    pl.run_scoped(finish, pltpu.VMEM((rows, cols), jnp.float32))

    remote(sto.at[pl.ds(0, 2)], sto.at[pl.ds(0, 2)], rb_send.at[8], rb_recv.at[0], me).wait_send()


def solution(mesh):
    n = mesh.shape["tp"]
    side = math.isqrt(n // 2)
    if side != len(OFFSETS) or n != 2 * side * side:
        raise ValueError("ring size")

    def block(x, w_gate, w_up, w_down):
        rows, cols = x.shape
        hidden = w_gate.shape[1]
        dma = pltpu.SemaphoreType.DMA
        chunks = hidden // LANES
        flops = 6 * n * rows * cols * hidden
        any_spec = pl.BlockSpec(memory_space=pl.ANY)
        out = pl.pallas_call(
            functools.partial(_kernel, side),
            out_shape=(
                pltpu.VMEM((rows, cols), x.dtype),
                jax.ShapeDtypeStruct((n, rows, cols), x.dtype),
                jax.ShapeDtypeStruct((13, rows, cols), x.dtype),
                jax.ShapeDtypeStruct((8, rows, cols), x.dtype),
                jax.ShapeDtypeStruct((10, rows // 2, cols), x.dtype),
            ),
            in_specs=[any_spec] * 4,
            out_specs=[pl.BlockSpec(memory_space=pltpu.VMEM)] + [any_spec] * 4,
            scratch_shapes=[
                pltpu.VMEM((hidden, cols), x.dtype),
                pltpu.VMEM((n, rows, hidden), x.dtype),
                pltpu.VMEM((2 * rows, cols), x.dtype),
                pltpu.VMEM((2, rows, cols), x.dtype),
                pltpu.VMEM((4, rows, cols), x.dtype),
                pltpu.VMEM((3, rows, cols), x.dtype),
                dma((2,)),
                dma((1,)),
                dma((26,)),
                dma((1,)),
                dma((4,)),
                dma((2,)),
                dma((5,)),
                dma((9,)),
                dma((8,)),
                dma((5,)),
                dma((10,)),
                dma((5,)),
                pltpu.SemaphoreType.REGULAR,
            ],
            compiler_params=pltpu.CompilerParams(
                collective_id=0, has_side_effects=True, vmem_limit_bytes=64_500_000
            ),
            cost_estimate=pl.CostEstimate(flops=flops, bytes_accessed=8 * n * rows * cols, transcendentals=0),
        )(x, w_gate, w_up, w_down)
        return out[0]

    return jax.shard_map(
        block,
        mesh=mesh,
        in_specs=(P(("dp", "tp"), None), P(None, "tp"), P(None, "tp"), P("tp", None)),
        out_specs=P(("dp", "tp"), None),
        check_vma=False,
    )
```
